512 devices in a mesh: grp: 2 (over y), gy: 32 (over z), gx: 4 (over x), gz: 2 (over core).
Axes of the slice: x: 4, y: 2, z: 32, core: 2. Of those that a mesh axis runs over, the one named last changes fastest.
The devices are a block of a 4x8x32 slice.
Arguments:
- pair: bfloat16 [1024, 512, 128], P(('grp', 'gx', 'gz'), 'gy'), parts along dimension 0, may hold values from -6 to 6
- lengths: int32 [2], P('grp'), parts along dimension 0, may hold values from 256 to 512
- ln_gain: float32 [128], replicated, may hold values from 0.1 to 1.9
- ln_bias: float32 [128], replicated, may hold values from -3 to 3
- w_ab: bfloat16 [128, 512], replicated, may hold values from -0.5 to 0.5
- w_gate: bfloat16 [128, 128], replicated, may hold values from -0.5 to 0.5
- out_gain: float32 [128], replicated, may hold values from 0.1 to 1.9
- out_bias: float32 [128], replicated, may hold values from -3 to 3
- w_out: bfloat16 [128, 128], replicated, may hold values from -0.5 to 0.5
Outputs:
- update: bfloat16 [1024, 512, 128], P(('grp', 'gx', 'gz'), 'gy'), parts along dimension 0
The draws below stay inside these ranges and needn't reach their ends.
There are 2 independent parts, one for each index of `grp`. The reference program is written for one: setup_inputs(seed, part) draws one part's arguments, and reference() takes and returns one part's arrays. A program takes and returns all parts, laid end to end along the dimension named above; an argument that names none is the same for every part. Nothing has to cross between parts.
Inputs may be any that keep to these rules, and one draw needn't show every extreme that they name: Residues from lengths[0] on are padding.
All inputs are finite; a program needn't handle non-finite values.
Results may differ from the reference program's by a relative error of at most 0.0052.
Values may be sent and summed in bfloat16 or wider, within the bound.
A program may use at most 128 MiB of HBM per device.

```python
import jax
import jax.numpy as jnp
from jax import lax

N = 512
C = 128
CH = 128


def shard_levels(key, dims, pieces, smallest, top_value):
    factor_of, own = 1.0, jax.random.fold_in(key, 6)
    for dim, parts in pieces:
        steps = jnp.exp(jax.random.uniform(jax.random.fold_in(own, dim), (parts,), jnp.float32, smallest / len(pieces), top_value / len(pieces)))
        factor_of = factor_of * jnp.repeat(steps, dims[dim] // parts).reshape([-1 if axis == dim else 1 for axis in range(len(dims))])
    return factor_of


def gaussian(rng, extent, scale, reach, pieces=(), kind=jnp.bfloat16):
    level = shard_levels(rng, extent, pieces, -0.22, 0.18) if pieces else 1.0
    array = jax.random.normal(rng, extent, jnp.float32) * scale * level
    return jnp.minimum(jnp.maximum(array, -reach), reach).astype(kind)


def setup_inputs(seed: int = 0, part: int = 0) -> dict:
    keys = jax.random.split(jax.random.key(seed), 10)
    part_keys = jax.random.split(jax.random.fold_in(keys[9], part), 10)
    pair = gaussian(part_keys[0], (N, N, C), 1.0, 6.0, ((0, 8), (1, 32)))
    lengths = jax.random.randint(part_keys[1], (1,), N // 2, N + 1).astype(jnp.int32)
    ln_gain = jnp.clip(1.0 + 0.18 * jax.random.normal(keys[2], (C,), jnp.float32), 0.1, 1.9)
    ln_bias = gaussian(keys[3], (C,), 0.5, 3.0, (), jnp.float32)
    w_ab = gaussian(keys[4], (C, 4 * CH), C ** -0.5, 0.5)
    w_gate = gaussian(keys[5], (C, C), C ** -0.5, 0.5)
    out_gain = jnp.clip(1.0 + 0.18 * jax.random.normal(keys[6], (CH,), jnp.float32), 0.1, 1.9)
    out_bias = gaussian(keys[7], (CH,), 0.5, 3.0, (), jnp.float32)
    w_out = gaussian(keys[8], (CH, C), CH ** -0.5, 0.5)
    return dict(pair=pair, lengths=lengths, ln_gain=ln_gain, ln_bias=ln_bias, w_ab=w_ab, w_gate=w_gate, out_gain=out_gain, out_bias=out_bias, w_out=w_out)


def layer_norm(values, gain, bias):
    values = values.astype(jnp.float32)
    mean = lax.optimization_barrier(jnp.mean(values, -1, keepdims=True))
    spread = lax.optimization_barrier(jnp.mean(jnp.square(values - mean), -1, keepdims=True))
    return (values - mean) * lax.rsqrt(spread + 1e-05) * gain.astype(jnp.float32) + bias.astype(jnp.float32)

def reference(pair, lengths, ln_gain, ln_bias, w_ab, w_gate, out_gain, out_bias, w_out):
    hidden = w_out.shape[0]
    width = pair.shape[2]
    normed = layer_norm(pair, ln_gain, ln_bias).astype(jnp.bfloat16)
    flat = normed.reshape(N * N, width)
    proj = jnp.dot(flat, w_ab, preferred_element_type=jnp.float32).reshape(N, N, 4 * hidden)
    live = (jnp.arange(N, dtype=jnp.int32) < lengths[0]).astype(jnp.float32)
    pair_mask = (live[:, None] * live[None, :])[..., None]
    left = (pair_mask * jax.nn.sigmoid(proj[..., :hidden]) * proj[..., hidden:2 * hidden]).astype(jnp.bfloat16)
    right = (pair_mask * jax.nn.sigmoid(proj[..., 2 * hidden:3 * hidden]) * proj[..., 3 * hidden:]).astype(jnp.bfloat16)
    triangle = jnp.einsum('ikc,jkc->ijc', left.astype(jnp.float32), right.astype(jnp.float32), precision=lax.Precision.HIGHEST)
    tri_norm = layer_norm(triangle, out_gain, out_bias).astype(jnp.bfloat16)
    gate = jax.nn.sigmoid(jnp.dot(flat, w_gate, preferred_element_type=jnp.float32))
    projected = jnp.dot(tri_norm.reshape(N * N, hidden), w_out, preferred_element_type=jnp.float32)
    return (gate * projected).astype(jnp.bfloat16).reshape(N, N, width)
```

```python
import functools

import jax
import jax.numpy as jnp
from jax import lax
from jax.experimental import pallas as pl
from jax.experimental.pallas import tpu as pltpu
from jax.sharding import PartitionSpec as P

MESH = pl.DeviceIdType.MESH
F32 = jnp.float32
BF16 = jnp.bfloat16


def kernel(
    dims,
    pair_ref,
    len_ref,
    ln_gain_ref,
    ln_bias_ref,
    w_ab_ref,
    w_gate_ref,
    out_gain_ref,
    out_bias_ref,
    w_out_ref,
    out_ref,
    norm_f32,
    buf_l,
    buf_r,
    gate_buf,
    send_l,
    send_r,
    recv_l,
    all_r,
    send_t,
    recv_t,
    y_buf,
    o_buf,
    wo_buf,
    gm_buf,
    bm_buf,
    send_sem,
    recv_sem,
):
    nz, nx, ng, rows, cols = dims
    nd = nx * ng
    z = lax.axis_index("gy")
    x = lax.axis_index("gx")
    g = lax.axis_index("gz")
    d_me = x * ng + g
    length = len_ref[0]
    half = 64

    barrier = pltpu.get_barrier_semaphore()
    for j in range(1, nz):
        pl.semaphore_signal(
            barrier, inc=1, device_id={"gy": lax.rem(z + j, nz)}, device_id_type=MESH
        )
    for j in range(1, nd):
        peer = lax.rem(d_me + j, nd)
        pl.semaphore_signal(
            barrier,
            inc=1,
            device_id={"gx": peer // ng, "gz": lax.rem(peer, ng)},
            device_id_type=MESH,
        )

    xs = pair_ref[...].astype(F32)
    mean = jnp.mean(xs, -1, keepdims=True)
    cen = xs - mean
    var = jnp.mean(cen * cen, -1, keepdims=True)
    normed = (cen * lax.rsqrt(var + 1e-05) * ln_gain_ref[...] + ln_bias_ref[...]).astype(BF16)
    norm_f32[...] = normed.astype(F32)
    gate_buf[...] = jax.nn.sigmoid(jnp.dot(normed, w_gate_ref[...], preferred_element_type=F32))

    w_t = w_ab_ref[...].T
    lane = lax.broadcasted_iota(jnp.int32, (1, 128), 1)
    lane_i = lax.rem(lane, half)
    lane_h = lane // half
    i_live = (d_me * rows + lane_i) < length
    for t in range(cols // 2):
        n_t = jnp.concatenate(
            [
                norm_f32[pl.ds(2 * t, rows, stride=cols), :],
                norm_f32[pl.ds(2 * t + 1, rows, stride=cols), :],
            ],
            axis=0,
        ).astype(BF16)
        proj = lax.dot_general(
            w_t, n_t, (((1,), (1,)), ((), ())), preferred_element_type=F32
        )
        k_live = (z * cols + 2 * t + lane_h) < length
        mask = jnp.where(jnp.logical_and(i_live, k_live), 1.0, 0.0)
        buf_l[pl.ds(t, 128, stride=8), :] = mask * jax.nn.sigmoid(proj[0:128]) * proj[128:256]
        buf_r[pl.ds(t, 128, stride=8), :] = mask * jax.nn.sigmoid(proj[256:384]) * proj[384:512]
    send_r[...] = buf_r[...].astype(BF16).reshape(send_r.shape)
    send_l[...] = buf_l[...].astype(BF16).reshape(send_l.shape)
    recv_l[z] = send_l[z]
    all_r[d_me, z] = send_r[z]

    pl.semaphore_wait(barrier, nz - 1 + nd - 1)

    offsets = []
    for j in range(nz // 2, 0, -1):
        offsets.append(j)
        if 2 * j != nz:
            offsets.append(nz - j)

    def to_z(src, dst, k, target):
        return pltpu.make_async_remote_copy(
            src, dst, send_sem.at[k], recv_sem.at[k], device_id={"gy": target}, device_id_type=MESH
        )

    for j in offsets:
        target = lax.rem(z + j, nz)
        to_z(send_r.at[target], all_r.at[d_me, z], 0, target).start()
    for j in offsets:
        target = lax.rem(z + j, nz)
        to_z(send_l.at[target], recv_l.at[z], 1, target).start()

    wo_buf[...] = w_out_ref[...].astype(F32)
    w2 = jnp.concatenate(
        [wo_buf[pl.ds(0, 64, stride=2), :], wo_buf[pl.ds(1, 64, stride=2), :]], axis=1
    ).astype(BF16)
    row_m = lax.broadcasted_iota(jnp.int32, (64, 128), 0)
    lane_c = lax.broadcasted_iota(jnp.int32, (64, 128), 1)
    for src, dst in ((out_gain_ref, gm_buf), (out_bias_ref, bm_buf)):
        vals = jnp.broadcast_to(src[...], (64, 128))
        even = jnp.sum(jnp.where(lane_c == 2 * row_m, vals, 0.0), 1, keepdims=True)
        odd = jnp.sum(jnp.where(lane_c == 2 * row_m + 1, vals, 0.0), 1, keepdims=True)
        dst[...] = jnp.where(lane_c < half, even, odd)

    to_z(send_r.at[pl.ds(0, nz - 1)], all_r.at[d_me, pl.ds(0, nz - 1)], 0, z).wait_recv()
    for j in range(1, nd):
        peer = lax.rem(d_me + j, nd)
        pltpu.make_async_remote_copy(
            all_r.at[d_me],
            all_r.at[d_me],
            send_sem.at[2],
            recv_sem.at[2],
            device_id={"gx": peer // ng, "gz": lax.rem(peer, ng)},
            device_id_type=MESH,
        ).start()
    to_z(send_l.at[pl.ds(0, nz - 1)], recv_l.at[pl.ds(0, nz - 1)], 1, z).wait_recv()
    to_z(all_r.at[pl.ds(0, nd - 1)], all_r.at[pl.ds(0, nd - 1)], 2, z).wait_recv()

    row_c2 = lax.rem(lax.broadcasted_iota(jnp.int32, (nz * 16, 128), 0) // 8, 2)
    lane64 = lax.broadcasted_iota(jnp.int32, (half, 128), 1)
    for cp in range(2):
        lp = recv_l[:, pl.ds(16 * cp, 16), :].reshape(nz * 16, 128)
        zero = jnp.zeros_like(lp)
        lz = jnp.concatenate(
            [jnp.where(row_c2 == 0, lp, zero), jnp.where(row_c2 == 1, lp, zero)], axis=1
        )
        for d in range(nd):
            rp = all_r[d, :, pl.ds(16 * cp, 16), :].reshape(nz * 16, 128)
            p = jnp.dot(rp.T, lz, preferred_element_type=F32)
            c0, c1 = p[:, 0:128], p[:, 128:256]
            a = jnp.where(lane64 < half, c0[0:64], c1[64:128])
            b = jnp.where(lane64 < half, c1[0:64], c0[64:128])
            tri = (a + pltpu.roll(b, half, 1)).astype(BF16)
            per = rows // cols
            send_t[pl.ds(d * per, per), pl.ds(16 * cp, 16), :] = tri.reshape(per, 16, 128)
    recv_t[z] = send_t[z]
    for j in offsets:
        target = lax.rem(z + j, nz)
        to_z(send_t.at[target], recv_t.at[z], 3, target).start()
    to_z(send_t.at[pl.ds(0, nz - 1)], recv_t.at[pl.ds(0, nz - 1)], 3, z).wait_recv()

    xt = recv_t[...].astype(F32).reshape(nz * 2, 16, 128)
    s = jnp.sum(xt, 0)
    mu = (s + pltpu.roll(s, half, 1)) * (1.0 / 128.0)
    ct = xt - mu
    v = jnp.sum(ct * ct, 0)
    rstd = lax.rsqrt((v + pltpu.roll(v, half, 1)) * (1.0 / 128.0) + 1e-05)
    for m in range(nz * 2):
        y = ct[m] * rstd * gm_buf[pl.ds(m, 1), :] + bm_buf[pl.ds(m, 1), :]
        y_buf[pl.ds(16 * m, 16), :] = y
    for j in range(cols):
        yj = y_buf[pl.ds(j, 64, stride=16), :].astype(BF16)
        p = jnp.dot(yj.T, w2, preferred_element_type=F32)
        o_buf[pl.ds(j, rows, stride=cols), :] = p[0:64, 0:128] + p[64:128, 128:256]
    out_ref[...] = (gate_buf[...] * o_buf[...]).astype(BF16)

    to_z(send_r.at[pl.ds(0, nz - 1)], all_r.at[d_me, pl.ds(0, nz - 1)], 0, z).wait_send()
    to_z(send_l.at[pl.ds(0, nz - 1)], recv_l.at[pl.ds(0, nz - 1)], 1, z).wait_send()
    to_z(all_r.at[pl.ds(0, nd - 1)], all_r.at[pl.ds(0, nd - 1)], 2, z).wait_send()
    to_z(send_t.at[pl.ds(0, nz - 1)], recv_t.at[pl.ds(0, nz - 1)], 3, z).wait_send()


def body(dims, pair, lengths, ln_gain, ln_bias, w_ab, w_gate, out_gain, out_bias, w_out):
    nz, nx, ng, rows, cols = dims
    nd = nx * ng
    flat = rows * cols
    width = pair.shape[2]
    vmem = pl.BlockSpec(memory_space=pltpu.VMEM)
    smem = pl.BlockSpec(memory_space=pltpu.SMEM)
    out = pl.pallas_call(
        functools.partial(kernel, dims),
        out_shape=jax.ShapeDtypeStruct((flat, width), BF16),
        in_specs=[vmem, smem] + [vmem] * 7,
        out_specs=vmem,
        scratch_shapes=[
            pltpu.VMEM((flat, 128), F32),
            pltpu.VMEM((1024, 128), F32),
            pltpu.VMEM((1024, 128), F32),
            pltpu.VMEM((flat, 128), F32),
            pltpu.VMEM((nz, 32, 128), BF16),
            pltpu.VMEM((nz, 32, 128), BF16),
            pltpu.VMEM((nz, 32, 128), BF16),
            pltpu.VMEM((nd, nz, 32, 128), BF16),
            pltpu.VMEM((nz, 32, 128), BF16),
            pltpu.VMEM((nz, 32, 128), BF16),
            pltpu.VMEM((1024, 128), F32),
            pltpu.VMEM((flat, 128), F32),
            pltpu.VMEM((128, 128), F32),
            pltpu.VMEM((64, 128), F32),
            pltpu.VMEM((64, 128), F32),
            pltpu.SemaphoreType.DMA((4,)),
            pltpu.SemaphoreType.DMA((4,)),
        ],
        compiler_params=pltpu.CompilerParams(
            collective_id=0, has_side_effects=True, vmem_limit_bytes=48 * 2**20
        ),
    )(
        pair.reshape(flat, width),
        lengths,
        ln_gain.reshape(1, -1),
        ln_bias.reshape(1, -1),
        w_ab,
        w_gate,
        out_gain.reshape(1, -1),
        out_bias.reshape(1, -1),
        w_out,
    )
    return out.reshape(pair.shape)


def solution(mesh):
    in_specs = (P(("grp", "gx", "gz"), "gy", None), P("grp"), P(), P(), P(), P(), P(), P(), P())
    out_specs = P(("grp", "gx", "gz"), "gy", None)

    def whole(pair, *rest):
        nz, nx, ng = mesh.shape["gy"], mesh.shape["gx"], mesh.shape["gz"]
        rows = pair.shape[0] // (mesh.shape["grp"] * nx * ng)
        cols = pair.shape[1] // nz
        dims = (nz, nx, ng, rows, cols)
        fn = jax.shard_map(
            functools.partial(body, dims),
            mesh=mesh,
            in_specs=in_specs,
            out_specs=out_specs,
            check_vma=False,
        )
        return fn(pair, *rest)

    return whole
```

```python
import functools

import jax
import jax.numpy as jnp
from jax import lax
from jax.experimental import pallas as pl
from jax.experimental.pallas import tpu as pltpu
from jax.sharding import PartitionSpec as P

MESH = pl.DeviceIdType.MESH
F32 = jnp.float32
BF16 = jnp.bfloat16


def kernel(
    dims,
    pair_hbm,
    len_ref,
    ln_gain_hbm,
    ln_bias_hbm,
    w_ab_hbm,
    w_gate_hbm,
    out_gain_hbm,
    out_bias_hbm,
    w_out_hbm,
    out_ref,
    pair_ref,
    ln_gain_ref,
    ln_bias_ref,
    out_gain_ref,
    out_bias_ref,
    w_ab_ref,
    w_gate_ref,
    w_out_ref,
    load_sem,
    norm_f32,
    buf,
    gate_buf,
    send_lr,
    all_lr,
    send_t,
    recv_t,
    y_buf,
    o_buf,
    send_sem,
    lr_sem,
    core_sem,
    t_sem,
    chain_sem,
    near_sem,
    in_sem,
):
    nz, nx, ng, rows, cols = dims
    nd = nx * ng
    owners = nz * nx
    z = lax.axis_index("gy")
    x = lax.axis_index("gx")
    g = lax.axis_index("gz")
    d_me = x * ng + g
    length = len_ref[0]
    q = lax.rem(z + nz - 1, nz)

    def z_of(place):
        return lax.rem(place + 1, nz)

    def signal(sem, target):
        pl.semaphore_signal(sem, inc=1, device_id=target, device_id_type=MESH)

    def remote(src, dst, k, sem, target):
        return pltpu.make_async_remote_copy(
            src, dst, send_sem.at[k], sem, device_id=target, device_id_type=MESH
        )

    offsets = []
    for j in range(nz // 2, 0, -1):
        offsets.append(j)
        if 2 * j != nz:
            offsets.append(nz - j)

    loads = [
        pltpu.make_async_copy(src, dst, load_sem.at[k])
        for k, (src, dst) in enumerate(
            (
                (pair_hbm, pair_ref),
                (w_ab_hbm, w_ab_ref),
                (w_gate_hbm, w_gate_ref),
                (w_out_hbm, w_out_ref),
                (ln_gain_hbm, ln_gain_ref),
                (ln_bias_hbm, ln_bias_ref),
                (out_gain_hbm, out_gain_ref),
                (out_bias_hbm, out_bias_ref),
            )
        )
    ]
    for load in loads:
        load.start()

    barrier = pltpu.get_barrier_semaphore()
    expect = nd - 1
    for step in (-2, -1, 1, 2):
        there = jnp.logical_and(q + step >= 0, q + step < nz)
        expect = expect + jnp.where(there, 1, 0)

        @pl.when(there)
        def _(step=step):
            signal(barrier, {"gy": z_of(q + step)})

    for j in range(1, nd):
        peer = lax.rem(d_me + j, nd)
        signal(barrier, {"gx": peer // ng, "gz": lax.rem(peer, ng)})
    loads[0].wait()
    loads[4].wait()
    loads[5].wait()
    xs = pair_ref[...].astype(F32)
    mean = jnp.mean(xs, -1, keepdims=True)
    cen = xs - mean
    var = jnp.mean(cen * cen, -1, keepdims=True)
    normed = (cen * lax.rsqrt(var + 1e-05) * ln_gain_ref[...] + ln_bias_ref[...]).astype(BF16)
    norm_f32[...] = normed.astype(F32)

    pl.semaphore_wait(barrier, expect)

    @pl.when(q < nz - 1)
    def _():
        signal(near_sem, {"gy": z_of(q + 1)})

    @pl.when(q >= 1)
    def _():
        pl.semaphore_wait(near_sem, 1)

    @pl.when(q >= 2)
    def _():
        pl.semaphore_wait(chain_sem, 1)

    @pl.when(q < nz - 2)
    def _():
        signal(chain_sem, {"gy": z_of(q + 2)})

    for j in offsets:
        other = lax.rem(q + j, nz)

        @pl.when(other < q)
        def _(other=other):
            signal(in_sem.at[q], {"gy": z_of(other)})

    loads[1].wait()
    w_t = w_ab_ref[...].T
    lane = lax.broadcasted_iota(jnp.int32, (1, 128), 1)
    row_live = (d_me * rows + lax.rem(lane, rows)) < length
    low = lax.broadcasted_iota(jnp.int32, (128, 128), 1) < rows
    for k in range(cols):
        n_k = norm_f32[pl.ds(k, rows, stride=cols), :]
        n_k = jnp.concatenate([n_k, n_k], axis=0).astype(BF16)
        proj = lax.dot_general(
            w_t, n_k, (((1,), (1,)), ((), ())), preferred_element_type=F32
        )
        mask = jnp.where(jnp.logical_and(row_live, z * cols + k < length), 1.0, 0.0)
        gate = jnp.where(low, proj[0:128], proj[256:384])
        value = jnp.where(low, proj[128:256], proj[384:512])
        buf[pl.ds(k, 128, stride=cols), :] = mask * jax.nn.sigmoid(gate) * value
    send_lr[...] = buf[...].astype(BF16).reshape(send_lr.shape)

    def send_to(place):
        for j in range(nx):
            xt = lax.rem(x + j, nx)
            remote(
                send_lr.at[z_of(place) * nx + xt],
                all_lr.at[g, x, q],
                0,
                lr_sem.at[q],
                {"gy": z_of(place), "gx": xt},
            ).start()

    for j in offsets:
        other = lax.rem(q + j, nz)

        @pl.when(other < q)
        def _(other=other):
            send_to(other)

    for j in range(1, nx):
        xt = lax.rem(x + j, nx)
        remote(
            send_lr.at[z * nx + xt], all_lr.at[g, x, q], 0, lr_sem.at[q], {"gx": xt}
        ).start()
    all_lr[g, x, q] = send_lr[z * nx + x]

    @pl.loop(q + 1, nz)
    def _(other):
        pl.semaphore_wait(in_sem.at[other], 1)
        send_to(other)

    loads[2].wait()
    gate_buf[...] = jax.nn.sigmoid(
        jnp.dot(norm_f32[...].astype(BF16), w_gate_ref[...], preferred_element_type=F32)
    )

    partner = {"gz": lax.rem(g + 1, ng)}
    per_group = 4
    for grp in range(nz // per_group):
        for s in range(grp * per_group, (grp + 1) * per_group):

            @pl.when(s != q)
            def _(s=s):
                part = all_lr.at[0, :, s]
                remote(part, part, 0, lr_sem.at[s], partner).wait_recv()

            @pl.when(s == q)
            def _(s=s):
                part = all_lr.at[0, pl.ds(0, nx - 1), s]
                remote(part, part, 0, lr_sem.at[s], partner).wait_recv()

        part = all_lr.at[g, :, pl.ds(grp * per_group, per_group)]
        remote(part, part, 1, core_sem, partner).start()
    remote(all_lr.at[0], all_lr.at[0], 1, core_sem, partner).wait_recv()

    right = []
    for d in range(nd):
        block = all_lr[d % ng, d // ng].reshape(nz * cols, 128)
        right.append(block.T[rows : 2 * rows])
    right = jnp.concatenate(right, axis=0)
    low8 = lax.broadcasted_iota(jnp.int32, (nz, 8, 128), 2) < rows
    for xt in range(nx):
        left = all_lr[g, xt].reshape(nz * cols, 128)
        tri = jnp.dot(right, left, preferred_element_type=F32).reshape(nz, 16, 128)
        turned = pltpu.roll(tri[:, 8:16].reshape(nz * 8, 128), rows, 1).reshape(nz, 8, 128)
        send_t[:, xt] = jnp.where(low8, tri[:, 0:8], turned).astype(BF16)

    for zt in range(nz):
        for j in range(nx):
            xt = lax.rem(x + j, nx)
            if j == 0:

                @pl.when(z != zt)
                def _(zt=zt, xt=xt):
                    remote(
                        send_t.at[zt, xt], recv_t.at[z * nx + x], 2, t_sem, {"gy": zt, "gx": xt}
                    ).start()
            else:
                remote(
                    send_t.at[zt, xt], recv_t.at[z * nx + x], 2, t_sem, {"gy": zt, "gx": xt}
                ).start()
    recv_t[z * nx + x] = send_t[z, x]

    others = recv_t.at[pl.ds(0, owners - 1)]
    remote(others, others, 2, t_sem, partner).wait_recv()

    for k in (3, 6, 7):
        loads[k].wait()
    ct = recv_t[...].astype(F32)
    ct = ct - jnp.sum(ct, 0) * (1.0 / owners)
    rstd = lax.rsqrt(jnp.sum(ct * ct, 0) * (1.0 / owners) + 1e-05)
    for c in range(owners):
        y_buf[pl.ds(8 * c, 8), :] = ct[c] * rstd * out_gain_ref[c] + out_bias_ref[c]
    w_out = w_out_ref[...]
    for j in range(8):
        yj = y_buf[pl.ds(j, owners, stride=8), :].astype(BF16)
        p = jnp.dot(yj.T, w_out, preferred_element_type=F32)
        o_buf[pl.ds(j, rows, stride=cols), :] = p[0:rows]
        o_buf[pl.ds(8 + j, rows, stride=cols), :] = p[rows : 2 * rows]
    out_ref[...] = (gate_buf[...] * o_buf[...]).astype(BF16)

    part = send_lr.at[pl.ds(0, owners - 1)]
    remote(part, part, 0, t_sem, partner).wait_send()
    remote(all_lr.at[0], all_lr.at[0], 1, t_sem, partner).wait_send()
    remote(others, others, 2, t_sem, partner).wait_send()


def body(dims, pair, lengths, ln_gain, ln_bias, w_ab, w_gate, out_gain, out_bias, w_out):
    nz, nx, ng, rows, cols = dims
    flat = rows * cols
    width = pair.shape[2]
    vmem = pl.BlockSpec(memory_space=pltpu.VMEM)
    hbm = pl.BlockSpec(memory_space=pltpu.HBM)
    smem = pl.BlockSpec(memory_space=pltpu.SMEM)
    out = pl.pallas_call(
        functools.partial(kernel, dims),
        out_shape=jax.ShapeDtypeStruct((flat, width), BF16),
        in_specs=[hbm, smem] + [hbm] * 7,
        out_specs=vmem,
        scratch_shapes=[
            pltpu.VMEM((flat, width), BF16),
            pltpu.VMEM((1, width), F32),
            pltpu.VMEM((1, width), F32),
            pltpu.SMEM((nz * nx,), F32),
            pltpu.SMEM((nz * nx,), F32),
            pltpu.VMEM(w_ab.shape, BF16),
            pltpu.VMEM(w_gate.shape, BF16),
            pltpu.VMEM(w_out.shape, BF16),
            pltpu.SemaphoreType.DMA((8,)),
            pltpu.VMEM((flat, 128), F32),
            pltpu.VMEM((128 * cols, 128), F32),
            pltpu.VMEM((flat, 128), F32),
            pltpu.VMEM((nz * nx, cols, 128), BF16),
            pltpu.VMEM((ng, nx, nz, cols, 128), BF16),
            pltpu.VMEM((nz, nx, 8, 128), BF16),
            pltpu.VMEM((nz * nx, 8, 128), BF16),
            pltpu.VMEM((nz * nx * 8, 128), F32),
            pltpu.VMEM((flat, 128), F32),
            pltpu.SemaphoreType.DMA((3,)),
            pltpu.SemaphoreType.DMA((nz,)),
            pltpu.SemaphoreType.DMA,
            pltpu.SemaphoreType.DMA,
            pltpu.SemaphoreType.REGULAR,
            pltpu.SemaphoreType.REGULAR,
            pltpu.SemaphoreType.REGULAR((nz,)),
        ],
        compiler_params=pltpu.CompilerParams(
            collective_id=0, has_side_effects=True, vmem_limit_bytes=60 * 1024 * 2**10
        ),
    )(
        pair.reshape(flat, width),
        lengths,
        ln_gain.reshape(1, -1),
        ln_bias.reshape(1, -1),
        w_ab,
        w_gate,
        out_gain,
        out_bias,
        w_out,
    )
    return out.reshape(pair.shape)


def solution(mesh):
    in_specs = (P(("grp", "gx", "gz"), "gy", None), P("grp"), P(), P(), P(), P(), P(), P(), P())
    out_specs = P(("grp", "gx", "gz"), "gy", None)

    def whole(pair, *rest):
        nz, nx, ng = mesh.shape["gy"], mesh.shape["gx"], mesh.shape["gz"]
        rows = pair.shape[0] // (mesh.shape["grp"] * nx * ng)
        cols = pair.shape[1] // nz
        dims = (nz, nx, ng, rows, cols)
        fn = jax.shard_map(
            functools.partial(body, dims),
            mesh=mesh,
            in_specs=in_specs,
            out_specs=out_specs,
            check_vma=False,
        )
        return fn(pair, *rest)

    return whole
```

```python
import functools

import jax
import jax.numpy as jnp
from jax import lax
from jax.experimental import pallas as pl
from jax.experimental.pallas import tpu as pltpu
from jax.sharding import PartitionSpec as P

MESH = pl.DeviceIdType.MESH
F32 = jnp.float32
BF16 = jnp.bfloat16


def kernel(
    dims,
    pair_hbm,
    len_ref,
    ln_gain_hbm,
    ln_bias_hbm,
    w_ab_hbm,
    w_gate_hbm,
    out_gain_hbm,
    out_bias_hbm,
    w_out_hbm,
    out_ref,
    pair_ref,
    ln_gain_ref,
    ln_bias_ref,
    out_gain_ref,
    out_bias_ref,
    w_ab_ref,
    w_gate_ref,
    w_out_ref,
    load_sem,
    norm_f32,
    buf,
    gate_buf,
    send_lr,
    all_lr,
    send_t,
    recv_t,
    y_buf,
    o_buf,
    send_sem,
    lr_sem,
    core_sem,
    t_sem,
    chain_sem,
    near_sem,
    in_sem,
):
    nz, nx, ng, rows, cols = dims
    nd = nx * ng
    owners = nz * nx
    z = lax.axis_index("gy")
    x = lax.axis_index("gx")
    g = lax.axis_index("gz")
    d_me = x * ng + g
    length = len_ref[0]
    q = lax.rem(z + nz - 1, nz)

    def z_of(place):
        return lax.rem(place + 1, nz)

    def signal(sem, target):
        pl.semaphore_signal(sem, inc=1, device_id=target, device_id_type=MESH)

    def remote(src, dst, k, sem, target):
        return pltpu.make_async_remote_copy(
            src, dst, send_sem.at[k], sem, device_id=target, device_id_type=MESH
        )

    offsets = []
    for j in range(nz // 2, 0, -1):
        offsets.append(j)
        if 2 * j != nz:
            offsets.append(nz - j)

    loads = [
        pltpu.make_async_copy(src, dst, load_sem.at[k])
        for k, (src, dst) in enumerate(
            (
                (pair_hbm, pair_ref),
                (w_ab_hbm, w_ab_ref),
                (w_gate_hbm, w_gate_ref),
                (w_out_hbm, w_out_ref),
                (ln_gain_hbm, ln_gain_ref),
                (ln_bias_hbm, ln_bias_ref),
                (out_gain_hbm, out_gain_ref),
                (out_bias_hbm, out_bias_ref),
            )
        )
    ]
    for load in loads:
        load.start()

    barrier = pltpu.get_barrier_semaphore()
    expect = nd - 1
    for step in (-2, -1, 1, 2):
        there = jnp.logical_and(q + step >= 0, q + step < nz)
        expect = expect + jnp.where(there, 1, 0)

        @pl.when(there)
        def _(step=step):
            signal(barrier, {"gy": z_of(q + step)})

    for j in range(1, nd):
        peer = lax.rem(d_me + j, nd)
        signal(barrier, {"gx": peer // ng, "gz": lax.rem(peer, ng)})
    loads[0].wait()
    loads[4].wait()
    loads[5].wait()
    xs = pair_ref[...].astype(F32)
    mean = jnp.mean(xs, -1, keepdims=True)
    cen = xs - mean
    var = jnp.mean(cen * cen, -1, keepdims=True)
    normed = (cen * lax.rsqrt(var + 1e-05) * ln_gain_ref[...] + ln_bias_ref[...]).astype(BF16)
    norm_f32[...] = normed.astype(F32)

    pl.semaphore_wait(barrier, expect)

    @pl.when(q < nz - 1)
    def _():
        signal(near_sem, {"gy": z_of(q + 1)})

    @pl.when(q >= 1)
    def _():
        pl.semaphore_wait(near_sem, 1)

    @pl.when(q >= 2)
    def _():
        pl.semaphore_wait(chain_sem, 1)

    @pl.when(q < nz - 2)
    def _():
        signal(chain_sem, {"gy": z_of(q + 2)})

    for j in offsets:
        other = lax.rem(q + j, nz)

        @pl.when(other < q)
        def _(other=other):
            signal(in_sem.at[q], {"gy": z_of(other)})

    loads[1].wait()
    w_t = w_ab_ref[...].T
    lane = lax.broadcasted_iota(jnp.int32, (1, 128), 1)
    row_live = (d_me * rows + lax.rem(lane, rows)) < length
    low = lax.broadcasted_iota(jnp.int32, (128, 128), 1) < rows
    for k in range(cols):
        n_k = norm_f32[pl.ds(k, rows, stride=cols), :]
        n_k = jnp.concatenate([n_k, n_k], axis=0).astype(BF16)
        proj = lax.dot_general(
            w_t, n_k, (((1,), (1,)), ((), ())), preferred_element_type=F32
        )
        mask = jnp.where(jnp.logical_and(row_live, z * cols + k < length), 1.0, 0.0)
        gate = jnp.where(low, proj[0:128], proj[256:384])
        value = jnp.where(low, proj[128:256], proj[384:512])
        buf[pl.ds(k, 128, stride=cols), :] = mask * jax.nn.sigmoid(gate) * value
    send_lr[...] = buf[...].astype(BF16).reshape(send_lr.shape)

    def send_to(place):
        for j in range(nx):
            xt = lax.rem(x + j, nx)
            remote(
                send_lr.at[z_of(place) * nx + xt],
                all_lr.at[g, x, q],
                0,
                lr_sem.at[q],
                {"gy": z_of(place), "gx": xt},
            ).start()

    for j in offsets:
        other = lax.rem(q + j, nz)

        @pl.when(other < q)
        def _(other=other):
            send_to(other)

    for j in range(1, nx):
        xt = lax.rem(x + j, nx)
        remote(
            send_lr.at[z * nx + xt], all_lr.at[g, x, q], 0, lr_sem.at[q], {"gx": xt}
        ).start()
    all_lr[g, x, q] = send_lr[z * nx + x]

    @pl.loop(q + 1, nz)
    def _(other):
        pl.semaphore_wait(in_sem.at[other], 1)
        send_to(other)

    loads[2].wait()
    gate_buf[...] = jax.nn.sigmoid(
        jnp.dot(norm_f32[...].astype(BF16), w_gate_ref[...], preferred_element_type=F32)
    )

    partner = {"gz": lax.rem(g + 1, ng)}
    per_group = 4
    for grp in range(nz // per_group):
        for s in range(grp * per_group, (grp + 1) * per_group):

            @pl.when(s != q)
            def _(s=s):
                part = all_lr.at[0, :, s]
                remote(part, part, 0, lr_sem.at[s], partner).wait_recv()

            @pl.when(s == q)
            def _(s=s):
                part = all_lr.at[0, pl.ds(0, nx - 1), s]
                remote(part, part, 0, lr_sem.at[s], partner).wait_recv()

        part = all_lr.at[g, :, pl.ds(grp * per_group, per_group)]
        remote(part, part, 1, core_sem, partner).start()
    remote(all_lr.at[0], all_lr.at[0], 1, core_sem, partner).wait_recv()

    right = []
    for d in range(nd):
        block = all_lr[d % ng, d // ng].reshape(nz * cols, 128)
        right.append(block.T[rows : 2 * rows])
    right = jnp.concatenate(right, axis=0)
    low8 = lax.broadcasted_iota(jnp.int32, (nz, 8, 128), 2) < rows
    for xt in range(nx):
        left = all_lr[g, xt].reshape(nz * cols, 128)
        tri = jnp.dot(right, left, preferred_element_type=F32).reshape(nz, 16, 128)
        turned = pltpu.roll(tri[:, 8:16].reshape(nz * 8, 128), rows, 1).reshape(nz, 8, 128)
        send_t[:, xt] = jnp.where(low8, tri[:, 0:8], turned).astype(BF16)

    for zt in [k // 2 + (k % 2) * (nz // 2) for k in range(nz)]:
        for j in range(nx):
            xt = lax.rem(x + j, nx)
            if j == 0:

                @pl.when(z != zt)
                def _(zt=zt, xt=xt):
                    remote(
                        send_t.at[zt, xt], recv_t.at[z * nx + x], 2, t_sem, {"gy": zt, "gx": xt}
                    ).start()
            else:
                remote(
                    send_t.at[zt, xt], recv_t.at[z * nx + x], 2, t_sem, {"gy": zt, "gx": xt}
                ).start()
    recv_t[z * nx + x] = send_t[z, x]

    others = recv_t.at[pl.ds(0, owners - 1)]
    remote(others, others, 2, t_sem, partner).wait_recv()

    for k in (3, 6, 7):
        loads[k].wait()
    ct = recv_t[...].astype(F32)
    ct = ct - jnp.sum(ct, 0) * (1.0 / owners)
    rstd = lax.rsqrt(jnp.sum(ct * ct, 0) * (1.0 / owners) + 1e-05)
    for c in range(owners):
        y_buf[pl.ds(8 * c, 8), :] = ct[c] * rstd * out_gain_ref[c] + out_bias_ref[c]
    w_out = w_out_ref[...]
    for j in range(8):
        yj = y_buf[pl.ds(j, owners, stride=8), :].astype(BF16)
        p = jnp.dot(yj.T, w_out, preferred_element_type=F32)
        o_buf[pl.ds(j, rows, stride=cols), :] = p[0:rows]
        o_buf[pl.ds(8 + j, rows, stride=cols), :] = p[rows : 2 * rows]
    out_ref[...] = (gate_buf[...] * o_buf[...]).astype(BF16)

    part = send_lr.at[pl.ds(0, owners - 1)]
    remote(part, part, 0, t_sem, partner).wait_send()
    remote(all_lr.at[0], all_lr.at[0], 1, t_sem, partner).wait_send()
    remote(others, others, 2, t_sem, partner).wait_send()


def body(dims, pair, lengths, ln_gain, ln_bias, w_ab, w_gate, out_gain, out_bias, w_out):
    nz, nx, ng, rows, cols = dims
    flat = rows * cols
    width = pair.shape[2]
    vmem = pl.BlockSpec(memory_space=pltpu.VMEM)
    hbm = pl.BlockSpec(memory_space=pltpu.HBM)
    smem = pl.BlockSpec(memory_space=pltpu.SMEM)
    def stay(a):
        return pltpu.with_memory_space_constraint(a, pltpu.HBM)

    out = pl.pallas_call(
        functools.partial(kernel, dims),
        out_shape=jax.ShapeDtypeStruct((flat, width), BF16),
        in_specs=[hbm, smem] + [hbm] * 7,
        out_specs=vmem,
        scratch_shapes=[
            pltpu.VMEM((flat, width), BF16),
            pltpu.VMEM((1, width), F32),
            pltpu.VMEM((1, width), F32),
            pltpu.SMEM((nz * nx,), F32),
            pltpu.SMEM((nz * nx,), F32),
            pltpu.VMEM(w_ab.shape, BF16),
            pltpu.VMEM(w_gate.shape, BF16),
            pltpu.VMEM(w_out.shape, BF16),
            pltpu.SemaphoreType.DMA((8,)),
            pltpu.VMEM((flat, 128), F32),
            pltpu.VMEM((128 * cols, 128), F32),
            pltpu.VMEM((flat, 128), F32),
            pltpu.VMEM((nz * nx, cols, 128), BF16),
            pltpu.VMEM((ng, nx, nz, cols, 128), BF16),
            pltpu.VMEM((nz, nx, 8, 128), BF16),
            pltpu.VMEM((nz * nx, 8, 128), BF16),
            pltpu.VMEM((nz * nx * 8, 128), F32),
            pltpu.VMEM((flat, 128), F32),
            pltpu.SemaphoreType.DMA((3,)),
            pltpu.SemaphoreType.DMA((nz,)),
            pltpu.SemaphoreType.DMA,
            pltpu.SemaphoreType.DMA,
            pltpu.SemaphoreType.REGULAR,
            pltpu.SemaphoreType.REGULAR,
            pltpu.SemaphoreType.REGULAR((nz,)),
        ],
        compiler_params=pltpu.CompilerParams(
            collective_id=0, has_side_effects=True, vmem_limit_bytes=48 * 2**20
        ),
    )(
        stay(pair.reshape(flat, width)),
        lengths,
        stay(ln_gain.reshape(1, -1)),
        stay(ln_bias.reshape(1, -1)),
        stay(w_ab),
        stay(w_gate),
        stay(out_gain),
        stay(out_bias),
        stay(w_out),
    )
    return out.reshape(pair.shape)


def solution(mesh):
    in_specs = (P(("grp", "gx", "gz"), "gy", None), P("grp"), P(), P(), P(), P(), P(), P(), P())
    out_specs = P(("grp", "gx", "gz"), "gy", None)

    def whole(pair, *rest):
        nz, nx, ng = mesh.shape["gy"], mesh.shape["gx"], mesh.shape["gz"]
        rows = pair.shape[0] // (mesh.shape["grp"] * nx * ng)
        cols = pair.shape[1] // nz
        dims = (nz, nx, ng, rows, cols)
        fn = jax.shard_map(
            functools.partial(body, dims),
            mesh=mesh,
            in_specs=in_specs,
            out_specs=out_specs,
            check_vma=False,
        )
        return fn(pair, *rest)

    return whole
```

```python
import functools

import jax
import jax.numpy as jnp
from jax import lax
from jax.experimental import pallas as pl
from jax.experimental.pallas import tpu as pltpu
from jax.sharding import PartitionSpec as P

MESH = pl.DeviceIdType.MESH
F32 = jnp.float32
BF16 = jnp.bfloat16


def kernel(
    dims,
    pair_hbm,
    len_ref,
    ln_gain_hbm,
    ln_bias_hbm,
    w_ab_hbm,
    w_gate_hbm,
    out_gain_hbm,
    out_bias_hbm,
    w_out_hbm,
    out_ref,
    pair_ref,
    ln_gain_ref,
    ln_bias_ref,
    out_gain_ref,
    out_bias_ref,
    w_ab_ref,
    w_gate_ref,
    w_out_ref,
    load_sem,
    norm_f32,
    buf,
    gate_buf,
    send_lr,
    all_lr,
    send_t,
    recv_t,
    y_buf,
    o_buf,
    send_sem,
    lr_sem,
    core_sem,
    t_sem,
    chain_sem,
    near_sem,
    in_sem,
):
    nz, nx, ng, rows, cols = dims
    nd = nx * ng
    owners = nz * nx
    z = lax.axis_index("gy")
    x = lax.axis_index("gx")
    g = lax.axis_index("gz")
    d_me = x * ng + g
    length = len_ref[0]
    q = lax.rem(z + nz - 1, nz)

    def z_of(place):
        return lax.rem(place + 1, nz)

    def signal(sem, target):
        pl.semaphore_signal(sem, inc=1, device_id=target, device_id_type=MESH)

    def remote(src, dst, k, sem, target):
        return pltpu.make_async_remote_copy(
            src, dst, send_sem.at[k], sem, device_id=target, device_id_type=MESH
        )

    offsets = []
    for j in range(nz // 2, 0, -1):
        offsets.append(j)
        if 2 * j != nz:
            offsets.append(nz - j)

    loads = [
        pltpu.make_async_copy(src, dst, load_sem.at[k])
        for k, (src, dst) in enumerate(
            (
                (pair_hbm, pair_ref),
                (w_ab_hbm, w_ab_ref),
                (w_gate_hbm, w_gate_ref),
                (w_out_hbm, w_out_ref),
                (ln_gain_hbm, ln_gain_ref),
                (ln_bias_hbm, ln_bias_ref),
                (out_gain_hbm, out_gain_ref),
                (out_bias_hbm, out_bias_ref),
            )
        )
    ]
    for load in loads:
        load.start()

    barrier = pltpu.get_barrier_semaphore()
    expect = nd - 1
    for step in (-2, -1, 1, 2):
        there = jnp.logical_and(q + step >= 0, q + step < nz)
        expect = expect + jnp.where(there, 1, 0)

        @pl.when(there)
        def _(step=step):
            signal(barrier, {"gy": z_of(q + step)})

    for j in range(1, nd):
        peer = lax.rem(d_me + j, nd)
        signal(barrier, {"gx": peer // ng, "gz": lax.rem(peer, ng)})
    loads[0].wait()
    loads[4].wait()
    loads[5].wait()
    xs = pair_ref[...].astype(F32)
    mean = jnp.mean(xs, -1, keepdims=True)
    cen = xs - mean
    var = jnp.mean(cen * cen, -1, keepdims=True)
    normed = (cen * lax.rsqrt(var + 1e-05) * ln_gain_ref[...] + ln_bias_ref[...]).astype(BF16)
    norm_f32[...] = normed.astype(F32)

    loads[1].wait()
    w_t = w_ab_ref[...].T
    lane = lax.broadcasted_iota(jnp.int32, (1, 128), 1)
    row_live = (d_me * rows + lax.rem(lane, rows)) < length
    low = lax.broadcasted_iota(jnp.int32, (128, 128), 1) < rows
    for k in range(cols):
        n_k = norm_f32[pl.ds(k, rows, stride=cols), :]
        n_k = jnp.concatenate([n_k, n_k], axis=0).astype(BF16)
        proj = lax.dot_general(
            w_t, n_k, (((1,), (1,)), ((), ())), preferred_element_type=F32
        )
        mask = jnp.where(jnp.logical_and(row_live, z * cols + k < length), 1.0, 0.0)
        gate = jnp.where(low, proj[0:128], proj[256:384])
        value = jnp.where(low, proj[128:256], proj[384:512])
        buf[pl.ds(k, 128, stride=cols), :] = mask * jax.nn.sigmoid(gate) * value
    send_lr[...] = buf[...].astype(BF16).reshape(send_lr.shape)

    pl.semaphore_wait(barrier, expect)

    @pl.when(q < nz - 1)
    def _():
        signal(near_sem, {"gy": z_of(q + 1)})

    @pl.when(q >= 1)
    def _():
        pl.semaphore_wait(near_sem, 1)

    @pl.when(q >= 2)
    def _():
        pl.semaphore_wait(chain_sem, 1)

    @pl.when(q < nz - 2)
    def _():
        signal(chain_sem, {"gy": z_of(q + 2)})

    for j in offsets:
        other = lax.rem(q + j, nz)

        @pl.when(other < q)
        def _(other=other):
            signal(in_sem.at[q], {"gy": z_of(other)})

    def send_to(place):
        for j in range(nx):
            xt = lax.rem(x + j, nx)
            remote(
                send_lr.at[z_of(place) * nx + xt],
                all_lr.at[g, x, q],
                0,
                lr_sem.at[q],
                {"gy": z_of(place), "gx": xt},
            ).start()

    for j in offsets:
        other = lax.rem(q + j, nz)

        @pl.when(other < q)
        def _(other=other):
            send_to(other)

    for j in range(1, nx):
        xt = lax.rem(x + j, nx)
        remote(
            send_lr.at[z * nx + xt], all_lr.at[g, x, q], 0, lr_sem.at[q], {"gx": xt}
        ).start()
    all_lr[g, x, q] = send_lr[z * nx + x]

    @pl.loop(q + 1, nz)
    def _(other):
        pl.semaphore_wait(in_sem.at[other], 1)
        send_to(other)

    loads[2].wait()
    gate_buf[...] = jax.nn.sigmoid(
        jnp.dot(norm_f32[...].astype(BF16), w_gate_ref[...], preferred_element_type=F32)
    )

    partner = {"gz": lax.rem(g + 1, ng)}
    per_group = 4
    for grp in range(nz // per_group):
        for s in range(grp * per_group, (grp + 1) * per_group):

            @pl.when(s != q)
            def _(s=s):
                part = all_lr.at[0, :, s]
                remote(part, part, 0, lr_sem.at[s], partner).wait_recv()

            @pl.when(s == q)
            def _(s=s):
                part = all_lr.at[0, pl.ds(0, nx - 1), s]
                remote(part, part, 0, lr_sem.at[s], partner).wait_recv()

        part = all_lr.at[g, :, pl.ds(grp * per_group, per_group)]
        remote(part, part, 1, core_sem, partner).start()
    remote(all_lr.at[0], all_lr.at[0], 1, core_sem, partner).wait_recv()

    right = []
    for d in range(nd):
        block = all_lr[d % ng, d // ng].reshape(nz * cols, 128)
        right.append(block.T[rows : 2 * rows])
    right = jnp.concatenate(right, axis=0)
    low8 = lax.broadcasted_iota(jnp.int32, (nz, 8, 128), 2) < rows
    for xt in range(nx):
        left = all_lr[g, xt].reshape(nz * cols, 128)
        tri = jnp.dot(right, left, preferred_element_type=F32).reshape(nz, 16, 128)
        turned = pltpu.roll(tri[:, 8:16].reshape(nz * 8, 128), rows, 1).reshape(nz, 8, 128)
        send_t[:, xt] = jnp.where(low8, tri[:, 0:8], turned).astype(BF16)

    for zt in [k // 2 + (k % 2) * (nz // 2) for k in range(nz)]:
        for j in range(nx):
            xt = lax.rem(x + j, nx)
            if j == 0:

                @pl.when(z != zt)
                def _(zt=zt, xt=xt):
                    remote(
                        send_t.at[zt, xt], recv_t.at[z * nx + x], 2, t_sem, {"gy": zt, "gx": xt}
                    ).start()
            else:
                remote(
                    send_t.at[zt, xt], recv_t.at[z * nx + x], 2, t_sem, {"gy": zt, "gx": xt}
                ).start()
    recv_t[z * nx + x] = send_t[z, x]

    others = recv_t.at[pl.ds(0, owners - 1)]
    remote(others, others, 2, t_sem, partner).wait_recv()

    for k in (3, 6, 7):
        loads[k].wait()
    ct = recv_t[...].astype(F32)
    ct = ct - jnp.sum(ct, 0) * (1.0 / owners)
    rstd = lax.rsqrt(jnp.sum(ct * ct, 0) * (1.0 / owners) + 1e-05)
    for c in range(owners):
        y_buf[pl.ds(8 * c, 8), :] = ct[c] * rstd * out_gain_ref[c] + out_bias_ref[c]
    w_out = w_out_ref[...]
    for j in range(8):
        yj = y_buf[pl.ds(j, owners, stride=8), :].astype(BF16)
        p = jnp.dot(yj.T, w_out, preferred_element_type=F32)
        o_buf[pl.ds(j, rows, stride=cols), :] = p[0:rows]
        o_buf[pl.ds(8 + j, rows, stride=cols), :] = p[rows : 2 * rows]
    out_ref[...] = (gate_buf[...] * o_buf[...]).astype(BF16)

    part = send_lr.at[pl.ds(0, owners - 1)]
    remote(part, part, 0, t_sem, partner).wait_send()
    remote(all_lr.at[0], all_lr.at[0], 1, t_sem, partner).wait_send()
    remote(others, others, 2, t_sem, partner).wait_send()


def body(dims, pair, lengths, ln_gain, ln_bias, w_ab, w_gate, out_gain, out_bias, w_out):
    nz, nx, ng, rows, cols = dims
    flat = rows * cols
    width = pair.shape[2]
    vmem = pl.BlockSpec(memory_space=pltpu.VMEM)
    hbm = pl.BlockSpec(memory_space=pltpu.HBM)
    smem = pl.BlockSpec(memory_space=pltpu.SMEM)
    def stay(a):
        return pltpu.with_memory_space_constraint(a, pltpu.HBM)

    out = pl.pallas_call(
        functools.partial(kernel, dims),
        out_shape=jax.ShapeDtypeStruct((flat, width), BF16),
        in_specs=[hbm, smem] + [hbm] * 7,
        out_specs=vmem,
        scratch_shapes=[
            pltpu.VMEM((flat, width), BF16),
            pltpu.VMEM((1, width), F32),
            pltpu.VMEM((1, width), F32),
            pltpu.SMEM((nz * nx,), F32),
            pltpu.SMEM((nz * nx,), F32),
            pltpu.VMEM(w_ab.shape, BF16),
            pltpu.VMEM(w_gate.shape, BF16),
            pltpu.VMEM(w_out.shape, BF16),
            pltpu.SemaphoreType.DMA((8,)),
            pltpu.VMEM((flat, 128), F32),
            pltpu.VMEM((128 * cols, 128), F32),
            pltpu.VMEM((flat, 128), F32),
            pltpu.VMEM((nz * nx, cols, 128), BF16),
            pltpu.VMEM((ng, nx, nz, cols, 128), BF16),
            pltpu.VMEM((nz, nx, 8, 128), BF16),
            pltpu.VMEM((nz * nx, 8, 128), BF16),
            pltpu.VMEM((nz * nx * 8, 128), F32),
            pltpu.VMEM((flat, 128), F32),
            pltpu.SemaphoreType.DMA((3,)),
            pltpu.SemaphoreType.DMA((nz,)),
            pltpu.SemaphoreType.DMA,
            pltpu.SemaphoreType.DMA,
            pltpu.SemaphoreType.REGULAR,
            pltpu.SemaphoreType.REGULAR,
            pltpu.SemaphoreType.REGULAR((nz,)),
        ],
        compiler_params=pltpu.CompilerParams(
            collective_id=0, has_side_effects=True, vmem_limit_bytes=48 * 2**20
        ),
    )(
        stay(pair.reshape(flat, width)),
        lengths,
        stay(ln_gain.reshape(1, -1)),
        stay(ln_bias.reshape(1, -1)),
        stay(w_ab),
        stay(w_gate),
        stay(out_gain),
        stay(out_bias),
        stay(w_out),
    )
    return out.reshape(pair.shape)


def solution(mesh):
    in_specs = (P(("grp", "gx", "gz"), "gy", None), P("grp"), P(), P(), P(), P(), P(), P(), P())
    out_specs = P(("grp", "gx", "gz"), "gy", None)

    def whole(pair, *rest):
        nz, nx, ng = mesh.shape["gy"], mesh.shape["gx"], mesh.shape["gz"]
        rows = pair.shape[0] // (mesh.shape["grp"] * nx * ng)
        cols = pair.shape[1] // nz
        dims = (nz, nx, ng, rows, cols)
        fn = jax.shard_map(
            functools.partial(body, dims),
            mesh=mesh,
            in_specs=in_specs,
            out_specs=out_specs,
            check_vma=False,
        )
        return fn(pair, *rest)

    return whole
```
